512 devices in a mesh: dp: 64 (over z_lo, y, core), expert: 8 (over z_hi, x).
Axes of the slice: x: 4, y: 4, z: 16 (z_hi: 2, z_lo: 8; z = z_hi * 8 + z_lo), core: 2. Of those that a mesh axis runs over, the one named last changes fastest.
Arguments:
- tokens: bfloat16 [1024, 6144], P('dp', 'expert'), may hold values from -6 to 6
- expert_ids: int32 [1024, 2], P('dp'), may hold values from 0 to 7, all different within a row; in each aligned block of 16 rows (0 to 15, 16 to 31, ...) at most 8 rows name the same one
- gate_probs: float32 [1024, 2], P('dp'), may hold values from 0.1 to 1
- w_gate: bfloat16 [8, 6144, 8192], P('expert', None, 'dp'), may hold values from -0.078125 to 0.078125
- w_up: bfloat16 [8, 6144, 8192], P('expert', None, 'dp'), may hold values from -0.078125 to 0.078125
- w_down_t: bfloat16 [8, 6144, 8192], P('expert', 'dp'), may hold values from -0.0625 to 0.0625
Outputs:
- mixed: bfloat16 [1024, 6144], P('dp', 'expert')
The draws below stay inside these ranges and needn't reach their ends.
Inputs may be any that keep to these rules, and one draw needn't show every extreme that they name: `expert_ids`: each row names 2 different experts. Among the 16 rows of one index of dp no expert is named more than 8 times, a bound that some block reaches.
All inputs are finite; a program needn't handle non-finite values.
Results may differ from the reference program's by a relative error of at most 0.0057.
Values may be sent and summed in bfloat16 or wider, within the bound.
No kernel may reach another device: no remote copies, remote signals or barrier semaphores. Data moves between devices by JAX's collectives and lax.ppermute only.
A program may use at most 64 MiB of HBM per device.

```python
import math
import jax
import jax.numpy as jnp
import numpy as np
from jax import lax

D = 6144
FF = 8192
EXPERTS = 8
TOP = 2
TOK_DEV = 16
CAP = 8
TOKENS = 1024
N_DP = 64


def shard_levels(stream_key, dims, pieces, smallest, high):
    factor_of = 1.0
    for dim, shards_of in pieces:
        steps = jax.random.uniform(jax.random.fold_in(jax.random.fold_in(stream_key, 6), dim), (shards_of,), jnp.float32, smallest / len(pieces), high / len(pieces))
        factor_of = factor_of * jnp.repeat(jnp.exp(steps), dims[dim] // shards_of).reshape((-1,) + (1,) * (len(dims) - 1 - dim))
    return factor_of


def deal_out(key, own, number, rows, count, top, most, lean):
    order = jax.random.permutation(key, count)
    packed, ordinary = load_shares(count, rows * top, most, lean, True), load_shares(count, rows * top, most, lean, False)
    places = jnp.arange(count)

    def named(tallies, turn):
        used = int((tallies > 0).sum())
        fixed = max(1, used // 4)
        passed = fixed + (places - fixed + turn * (used - fixed)) % max(1, count - fixed)
        return jnp.zeros((count,), jnp.int32).at[order[jnp.where(places < fixed, places, passed)]].set(jnp.asarray(tallies, jnp.int32))

    tallies = jnp.where(number % 4 == 0, named(packed, number // 4), named(ordinary, number - number // 4 - 1))
    mixed = jax.random.permutation(jax.random.fold_in(own, 3), count)
    source_of, taker = mixed[0:count // 2 * 2:2], mixed[1:count // 2 * 2:2]
    slack = jnp.minimum(tallies[source_of] - 1, most - tallies[taker]) // 2
    slack = jnp.where((source_of == order[0]) | (taker == order[0]) | (tallies[taker] == 0), 0, jnp.maximum(slack, 0))
    passed = jax.random.randint(jax.random.fold_in(own, 4), (count // 2,), 0, 1 << 20) % (slack + 1)
    tallies = tallies.at[source_of].add(-passed).at[taker].add(passed)
    labels = jnp.searchsorted(jnp.cumsum(tallies), jnp.arange(rows * top), side="right").astype(jnp.int32)
    table = labels.reshape(top, rows).T
    table = table[jax.random.permutation(jax.random.fold_in(own, 1), rows)]
    turn = jax.random.randint(jax.random.fold_in(own, 2), (rows, 1), 0, top)
    return jnp.take_along_axis(table, (jnp.arange(top)[None, :] + turn) % top, axis=1)


def load_shares(number_of, total, limit, skew, full):
    portions = [(1 << 20) // math.isqrt(standing ** skew) + 1 for standing in range(1, number_of + 1)]
    largest = limit if full else min(limit, max(-(-total // number_of), total * portions[0] // sum(portions)))
    least = 1 if total - largest >= number_of - 1 else 0
    counts, rest = [largest] + [least] * (number_of - 1), total - largest - least * (number_of - 1)
    while rest > 0:
        free = [i for i in range(1, number_of) if counts[i] < largest] or [i for i in range(1, number_of) if counts[i] < limit]
        pool, remaining = sum([portions[i] for i in free]), rest
        for i in free:
            more = min(limit - counts[i], max(1, remaining * portions[i] // pool), rest)
            counts[i] = counts[i] + more
            rest = rest - more
    return np.array(counts)


def normal_values(own_key, shape, spread, limit, split=(), kind=jnp.bfloat16):
    array = spread * jax.random.normal(own_key, shape, jnp.float32)
    if split:
        array = array * shard_levels(own_key, shape, split, -0.22, 0.18)
    return jnp.clip(array, -limit, limit).astype(kind)


def setup_inputs(seed: int = 0) -> dict:
    key_list = jax.random.split(jax.random.key(seed), 7)
    tokens = normal_values(key_list[0], (TOKENS, D), 1.0, 6.0, ((0, 64), (1, 8)))
    expert_ids_keys = jax.random.split(jax.random.fold_in(key_list[1], 1), TOKENS // TOK_DEV)
    expert_ids_turns = jax.random.permutation(jax.random.fold_in(key_list[1], 3), TOKENS // TOK_DEV)
    expert_ids = jax.vmap(lambda own, number: deal_out(jax.random.fold_in(key_list[1], 2), own, number, TOK_DEV, EXPERTS, TOP, CAP, 2))(expert_ids_keys, expert_ids_turns).reshape((TOKENS, TOP))
    gate_probs = jnp.clip(jnp.exp(math.log(1.0) - 2.3025851 * jax.random.uniform(key_list[2], (TOKENS, TOP), jnp.float32) ** shard_levels(key_list[2], (TOKENS, TOP), ((0, 64),), -0.2, 0.2)), 0.1, 1.0)
    w_gate = normal_values(key_list[3], (EXPERTS, D, FF), D ** -0.5, 0.078125, ((0, 8), (2, 64)))
    w_up = normal_values(key_list[4], (EXPERTS, D, FF), D ** -0.5, 0.078125, ((0, 8), (2, 64)))
    w_down_t = normal_values(key_list[5], (EXPERTS, D, FF), FF ** -0.5, 0.0625, ((0, 8), (1, 64)))
    return dict(tokens=tokens, expert_ids=expert_ids, gate_probs=gate_probs, w_gate=w_gate, w_up=w_up, w_down_t=w_down_t)


def positions(expert_ids):
    blocks = expert_ids.reshape(N_DP, TOK_DEV * TOP)
    onehot = (blocks[:, :, None] == jnp.arange(EXPERTS, dtype=jnp.int32)[None, None, :]).astype(jnp.int32)
    earlier = jnp.cumsum(onehot, axis=1) - onehot
    return jnp.sum(earlier * onehot, axis=2).reshape(TOKENS, TOP).astype(jnp.int32)


def one_expert(operands):
    rows, gate_w, up_w, down_w = operands
    gate = jnp.dot(rows, gate_w, preferred_element_type=jnp.float32)
    up = jnp.dot(rows, up_w, preferred_element_type=jnp.float32)
    hidden = (jax.nn.silu(gate) * up).astype(jnp.bfloat16)
    result = lax.dot_general(hidden, down_w, (((1,), (1,)), ((), ())), preferred_element_type=jnp.float32)
    return result.astype(jnp.bfloat16)


def reference(tokens, expert_ids, gate_probs, w_gate, w_up, w_down_t):
    position = positions(expert_ids)
    block_of = (jnp.arange(TOKENS, dtype=jnp.int32) // TOK_DEV).astype(jnp.int32)
    block_rep = jnp.repeat(block_of, TOP)
    flat_ids = expert_ids.reshape(-1).astype(jnp.int32)
    flat_pos = position.reshape(-1).astype(jnp.int32)
    dispatched = jnp.zeros((EXPERTS, N_DP, CAP, D), jnp.bfloat16)
    dispatched = dispatched.at[flat_ids, block_rep, flat_pos].set(jnp.repeat(tokens, TOP, axis=0))
    expert_out = lax.map(one_expert, (dispatched.reshape(EXPERTS, N_DP * CAP, D), w_gate, w_up, w_down_t))
    expert_out = expert_out.reshape(EXPERTS, N_DP, CAP, D)
    picked = expert_out[flat_ids, block_rep, flat_pos].reshape(TOKENS, TOP, D).astype(jnp.float32)
    mixed = jnp.sum(gate_probs[:, :, None] * picked, axis=1)
    return mixed.astype(jnp.bfloat16)
```

```python
import jax
import jax.numpy as jnp
from jax import lax
from jax.sharding import Mesh, PartitionSpec as P

AXES = ("zl", "y", "c", "zh", "x")
SIZES = (8, 4, 2, 2, 4)
SWAP = [(0, 1), (1, 0)]


def everyone(value, axis, count):
    return lax.all_to_all(
        jnp.broadcast_to(value[None], (count,) + value.shape), axis, 0, 0, tiled=True
    )


def slot_numbers(expert_ids, capacity):
    flat = expert_ids.reshape(-1)
    pairs = flat.shape[0]
    same = flat[:, None] == flat[None, :]
    index = jnp.arange(pairs, dtype=jnp.int32)
    earlier = index[None, :] < index[:, None]
    position = jnp.sum((same & earlier).astype(jnp.int32), axis=1)
    return (flat * capacity + position).reshape(expert_ids.shape)


def per_device(tokens, expert_ids, gate_probs, w_gate, w_up, w_down_t):
    zl, y, c, zh, x = SIZES
    block, width = tokens.shape
    capacity = block // 2
    experts = zh * x
    model = width * experts
    units = w_gate.shape[2]
    f32, bf16 = jnp.float32, jnp.bfloat16

    gate_own, up_own = w_gate[0], w_up[0]
    gate_far = lax.ppermute(gate_own, "c", SWAP)
    up_far = lax.ppermute(up_own, "c", SWAP)
    features = w_down_t.shape[1]
    down = w_down_t[0].reshape(features, zl, y, c * units).transpose(2, 0, 1, 3)
    down = lax.all_to_all(
        down.reshape(y, features, zl * c * units), "y", 0, 0, tiled=True
    ).reshape(y * features, zl * c * units)
    down_far = lax.ppermute(down, "c", SWAP)

    slot = slot_numbers(expert_ids, capacity)
    tail = jnp.pad(slot, ((0, 0), (0, 126)), constant_values=0).astype(bf16)
    seen = everyone(jnp.concatenate([tokens, tail], axis=1), ("zh", "zl"), zh * zl)
    seen = seen.reshape(zh, zl * block, width + 128)
    slot_seen = seen[0, :, width : width + 2].astype(f32).astype(jnp.int32)

    rows = zl * capacity
    wanted = (
        lax.axis_index("zh") * (x * capacity)
        + jnp.arange(x, dtype=jnp.int32)[:, None, None] * capacity
        + jnp.arange(capacity, dtype=jnp.int32)[None, None, :]
        + jnp.zeros((1, zl, 1), jnp.int32)
    ).reshape(-1)
    row_block = (jnp.arange(x * rows, dtype=jnp.int32) // capacity) % zl
    token_block = jnp.arange(zl * block, dtype=jnp.int32) // block
    hit = (slot_seen[:, 0][None, :] == wanted[:, None]) | (
        slot_seen[:, 1][None, :] == wanted[:, None]
    )
    hit = (hit & (row_block[:, None] == token_block[None, :])).astype(bf16)
    slots = jnp.concatenate(
        [
            jnp.dot(hit, seen[h, :, :width], preferred_element_type=f32)
            .astype(bf16)
            .reshape(x, rows, width)
            for h in range(zh)
        ],
        axis=1,
    )
    arrived = lax.all_to_all(slots, "x", 0, 0, tiled=True)
    piece = jnp.concatenate(
        [arrived[i, h * rows : (h + 1) * rows] for h in range(zh) for i in range(x)],
        axis=1,
    )
    piece = everyone(piece, "y", y).reshape(y * rows, model)

    def act(w1, w2):
        gate = jnp.dot(piece, w1, preferred_element_type=f32)
        up = jnp.dot(piece, w2, preferred_element_type=f32)
        return (jax.nn.silu(gate) * up).astype(bf16)

    first = lax.axis_index("c") == 0
    own, far = act(gate_own, up_own), act(gate_far, up_far)
    hidden = jnp.concatenate(
        [jnp.where(first, own, far), jnp.where(first, far, own)], axis=1
    )
    hidden = everyone(hidden, "zl", zl)
    hidden = hidden.transpose(1, 0, 2).reshape(y * rows, zl * c * units)

    def out(w):
        part = lax.dot_general(
            hidden, w, (((1,), (1,)), ((), ())), preferred_element_type=f32
        )
        return part.astype(bf16)

    own, far = out(down), out(down_far)
    part = jnp.concatenate(
        [jnp.where(first, own, far), jnp.where(first, far, own)], axis=1
    ).reshape(y, rows, width)
    part = lax.all_to_all(part, "y", 0, 0, tiled=True).astype(f32)
    result = ((part[0] + part[1]) + (part[2] + part[3])).astype(bf16)

    result = lax.all_to_all(
        result.reshape(zl, capacity, width), "zl", 0, 0, tiled=True
    )
    result = lax.all_to_all(result, ("zh", "x"), 0, 0, tiled=True)
    result = result.reshape(experts * capacity, width)

    every = jnp.arange(experts * capacity, dtype=jnp.int32)
    mixed = 0.0
    for k in range(2):
        pick = (slot[:, k][:, None] == every[None, :]).astype(bf16)
        picked = jnp.dot(pick, result, preferred_element_type=f32)
        mixed = mixed + gate_probs[:, k][:, None] * picked
    mixed = mixed.astype(bf16).reshape(block, c, y, features)
    return mixed.transpose(0, 2, 1, 3).reshape(block, width)


def solution(mesh):
    physical = Mesh(mesh.devices.reshape(SIZES), AXES)
    dp, expert = AXES[:3], AXES[3:]
    placed = (
        P(dp, expert),
        P(dp, None),
        P(dp, None),
        P(expert, None, dp),
        P(expert, None, dp),
        P(expert, dp, None),
    )
    return jax.shard_map(
        per_device,
        mesh=physical,
        in_specs=placed,
        out_specs=P(dp, expert),
        check_vma=False,
    )
```

```python
import jax
import jax.numpy as jnp
from jax import lax
from jax.sharding import Mesh, PartitionSpec as P

AXES = ("zl", "y", "c", "zh", "x")
SIZES = (8, 4, 2, 2, 4)
SWAP = [(0, 1), (1, 0)]


def step(count, shift):
    return [(i, (i + shift) % count) for i in range(count)]


def flip(axis_size, mask):
    return [(i, i ^ mask) for i in range(axis_size)]


def everyone(value, axis, count):
    return lax.all_to_all(
        jnp.broadcast_to(value[None], (count,) + value.shape), axis, 0, 0, tiled=True
    )


def slot_numbers(expert_ids, capacity):
    flat = expert_ids.reshape(-1)
    pairs = flat.shape[0]
    same = flat[:, None] == flat[None, :]
    index = jnp.arange(pairs, dtype=jnp.int32)
    earlier = index[None, :] < index[:, None]
    position = jnp.sum((same & earlier).astype(jnp.int32), axis=1)
    return (flat * capacity + position).reshape(expert_ids.shape)


def per_device(tokens, expert_ids, gate_probs, w_gate, w_up, w_down_t):
    zl, y, c, zh, x = SIZES
    block, width = tokens.shape
    capacity = block // 2
    experts = zh * x
    model = width * experts
    units = w_gate.shape[2]
    f32, bf16 = jnp.float32, jnp.bfloat16

    gate_own, up_own = w_gate[0], w_up[0]
    gate_far = lax.ppermute(gate_own, "c", SWAP)
    up_far = lax.ppermute(up_own, "c", SWAP)
    features = w_down_t.shape[1]
    z_here = lax.axis_index("zl")
    order = [q ^ k for k in range(4) for q in (0, 4)]
    span = c * units
    y_here = lax.axis_index("y")

    def columns(shift):
        at = ((y_here + shift) % y) * span
        return jnp.concatenate(
            [
                lax.dynamic_slice_in_dim(
                    w_down_t[0], (z_here ^ j) * (y * span) + at, span, 1
                )
                for j in order
            ],
            axis=1,
        )

    down = jnp.zeros((y, features, zl * span), bf16)
    for k in range(y):
        moved = columns(k)
        if k:
            moved = lax.ppermute(moved, "y", step(y, k))
        down = lax.dynamic_update_slice_in_dim(down, moved[None], (y_here - k) % y, 0)
    down = down.reshape(y * features, zl * span)
    slot = slot_numbers(expert_ids, capacity)
    tail = jnp.pad(slot, ((0, 0), (0, 126)), constant_values=0).astype(bf16)
    seen = everyone(jnp.concatenate([tokens, tail], axis=1), ("zh", "zl"), zh * zl)
    seen = seen.reshape(zh, zl * block, width + 128)
    slot_seen = seen[0, :, width : width + 2].astype(f32).astype(jnp.int32)

    rows = zl * capacity
    wanted = (
        lax.axis_index("zh") * (x * capacity)
        + jnp.arange(x, dtype=jnp.int32)[:, None, None] * capacity
        + jnp.arange(capacity, dtype=jnp.int32)[None, None, :]
        + jnp.zeros((1, zl, 1), jnp.int32)
    ).reshape(-1)
    row_block = (jnp.arange(x * rows, dtype=jnp.int32) // capacity) % zl
    token_block = jnp.arange(zl * block, dtype=jnp.int32) // block
    hit = (slot_seen[:, 0][None, :] == wanted[:, None]) | (
        slot_seen[:, 1][None, :] == wanted[:, None]
    )
    hit = (hit & (row_block[:, None] == token_block[None, :])).astype(bf16)
    slots = jnp.concatenate(
        [
            jnp.dot(hit, seen[h, :, :width], preferred_element_type=f32)
            .astype(bf16)
            .reshape(x, rows, width)
            for h in range(zh)
        ],
        axis=1,
    )
    arrived = lax.all_to_all(slots, "x", 0, 0, tiled=True)
    arrived, down, gate_far, up_far = lax.optimization_barrier(
        (arrived, down, gate_far, up_far)
    )
    piece = jnp.concatenate(
        [arrived[i, h * rows : (h + 1) * rows] for h in range(zh) for i in range(x)],
        axis=1,
    )
    down_far = lax.ppermute(down, "c", SWAP)
    up1 = lax.ppermute(piece, "y", step(y, 1))
    dn1 = lax.ppermute(piece, "y", step(y, -1))
    half = rows // 2
    far_a = lax.ppermute(up1[:half], "y", step(y, 1))
    far_b = lax.ppermute(dn1[half:], "y", step(y, -1))
    blocks = (piece, up1, dn1, jnp.concatenate([far_a, far_b], axis=0))
    first = lax.axis_index("c") == 0

    def act(rows_in, w1, w2):
        gate = jnp.dot(rows_in, w1, preferred_element_type=f32)
        up = jnp.dot(rows_in, w2, preferred_element_type=f32)
        return (jax.nn.silu(gate) * up).astype(bf16)

    def out(hidden, w):
        total = 0.0
        for k, h in enumerate(hidden):
            total = total + lax.dot_general(
                h,
                w[:, k * 2 * span : (k + 1) * 2 * span],
                (((1,), (1,)), ((), ())),
                preferred_element_type=f32,
            )
        return total.astype(bf16)

    taken = jnp.concatenate(blocks, axis=0)
    own, far = act(taken, gate_own, up_own), act(taken, gate_far, up_far)
    hidden = jnp.concatenate(
        [jnp.where(first, own, far), jnp.where(first, far, own)], axis=1
    )
    other = lax.ppermute(hidden, "zl", flip(zl, 4))
    pair = jnp.concatenate([hidden, other], axis=1)
    pairs = [pair] + [lax.ppermute(pair, "zl", flip(zl, k)) for k in (1, 2, 3)]
    own, far = out(pairs, down), out(pairs, down_far)
    part = jnp.concatenate(
        [jnp.where(first, own, far), jnp.where(first, far, own)], axis=1
    )
    parts = [part[n * rows : (n + 1) * rows] for n in range(y)]

    part = jnp.stack([parts[0], parts[2], parts[3], parts[1]])
    part = lax.dynamic_slice_in_dim(
        jnp.concatenate([part, part]), (y - y_here) % y, y, 0
    )
    part = lax.all_to_all(part, "y", 0, 0, tiled=True).astype(f32)
    result = ((part[0] + part[1]) + (part[2] + part[3])).astype(bf16)

    result = lax.all_to_all(
        result.reshape(zl, capacity, width), "zl", 0, 0, tiled=True
    )
    result = lax.all_to_all(result, ("zh", "x"), 0, 0, tiled=True)
    result, slot, gate_probs = lax.optimization_barrier((result, slot, gate_probs))
    result = result.reshape(experts * capacity, width)

    every = jnp.arange(experts * capacity, dtype=jnp.int32)
    mixed = 0.0
    for k in range(2):
        pick = (slot[:, k][:, None] == every[None, :]).astype(bf16)
        picked = jnp.dot(pick, result, preferred_element_type=f32)
        mixed = mixed + gate_probs[:, k][:, None] * picked
    mixed = mixed.astype(bf16).reshape(block, c, y, features)
    return mixed.transpose(0, 2, 1, 3).reshape(block, width)


def solution(mesh):
    physical = Mesh(mesh.devices.reshape(SIZES), AXES)
    dp, expert = AXES[:3], AXES[3:]
    placed = (
        P(dp, expert),
        P(dp, None),
        P(dp, None),
        P(expert, None, dp),
        P(expert, None, dp),
        P(expert, dp, None),
    )
    return jax.shard_map(
        per_device,
        mesh=physical,
        in_specs=placed,
        out_specs=P(dp, expert),
        check_vma=False,
    )
```

```python
import jax
import jax.numpy as jnp
from jax import lax
from jax.experimental import pallas as pl
from jax.experimental.pallas import tpu as pltpu
from jax.sharding import Mesh, PartitionSpec as P

AXES = ("zl", "y", "c", "zh", "x")
SIZES = (8, 4, 2, 2, 4)
SWAP = [(0, 1), (1, 0)]


def step(count, shift):
    return [(i, (i + shift) % count) for i in range(count)]


def flip(axis_size, mask):
    return [(i, i ^ mask) for i in range(axis_size)]


def everyone(value, axis, count):
    return lax.all_to_all(
        jnp.broadcast_to(value[None], (count,) + value.shape), axis, 0, 0, tiled=True
    )


def slot_numbers(expert_ids, capacity):
    flat = expert_ids.reshape(-1)
    pairs = flat.shape[0]
    same = flat[:, None] == flat[None, :]
    index = jnp.arange(pairs, dtype=jnp.int32)
    earlier = index[None, :] < index[:, None]
    position = jnp.sum((same & earlier).astype(jnp.int32), axis=1)
    return (flat * capacity + position).reshape(expert_ids.shape)


DEPTH = 768


def gated_kernel(core_ref, rows_ref, g0, u0, g1, u1, out_ref, gate, up):
    at = pl.program_id(0)

    @pl.when(at == 0)
    def _():
        gate[...] = jnp.zeros_like(gate)
        up[...] = jnp.zeros_like(up)

    lhs = rows_ref[...]
    w_g = jnp.concatenate([g0[...], g1[...]], axis=1)
    w_u = jnp.concatenate([u0[...], u1[...]], axis=1)
    gate[...] += jnp.dot(lhs, w_g, preferred_element_type=jnp.float32)
    up[...] += jnp.dot(lhs, w_u, preferred_element_type=jnp.float32)

    @pl.when(at == pl.num_programs(0) - 1)
    def _():
        g = gate[...]
        value = (g / (1.0 + jnp.exp(-g)) * up[...]).astype(out_ref.dtype)
        n = value.shape[1] // 2

        @pl.when(core_ref[0] == 0)
        def _():
            out_ref[...] = value

        @pl.when(core_ref[0] != 0)
        def _():
            out_ref[...] = jnp.concatenate([value[:, n:], value[:, :n]], axis=1)


def gated(core, rows, g0, u0, g1, u1):
    m, depth = rows.shape
    units = g0.shape[1]
    weight = pl.BlockSpec((DEPTH, units), lambda i, core: (i, 0))
    return pl.pallas_call(
        gated_kernel,
        out_shape=jax.ShapeDtypeStruct((m, 2 * units), rows.dtype),
        grid_spec=pltpu.PrefetchScalarGridSpec(
            num_scalar_prefetch=1,
            grid=(depth // DEPTH,),
            in_specs=[pl.BlockSpec((m, DEPTH), lambda i, core: (0, i))] + [weight] * 4,
            out_specs=pl.BlockSpec((m, 2 * units), lambda i, core: (0, 0)),
            scratch_shapes=[
                pltpu.VMEM((m, 2 * units), jnp.float32),
                pltpu.VMEM((m, 2 * units), jnp.float32),
            ],
        ),
        compiler_params=pltpu.CompilerParams(dimension_semantics=("arbitrary",)),
        cost_estimate=pl.CostEstimate(
            flops=2 * m * depth * units * 4,
            transcendentals=m * units * 2,
            bytes_accessed=depth * (m + 4 * units) * 2,
        ),
        name="gated",
    )(core, rows, g0, u0, g1, u1)


def per_device(tokens, expert_ids, gate_probs, w_gate, w_up, w_down_t):
    zl, y, c, zh, x = SIZES
    block, width = tokens.shape
    capacity = block // 2
    experts = zh * x
    model = width * experts
    units = w_gate.shape[2]
    f32, bf16 = jnp.float32, jnp.bfloat16

    gate_own, up_own = w_gate[0], w_up[0]
    gate_far = lax.ppermute(gate_own, "c", SWAP)
    up_far = lax.ppermute(up_own, "c", SWAP)
    features = w_down_t.shape[1]
    z_here = lax.axis_index("zl")
    order = [q ^ k for k in range(4) for q in (0, 4)]
    span = c * units
    y_here = lax.axis_index("y")

    def columns(shift):
        at = ((y_here + shift) % y) * span
        return jnp.concatenate(
            [
                lax.dynamic_slice_in_dim(
                    w_down_t[0], (z_here ^ j) * (y * span) + at, span, 1
                )
                for j in order
            ],
            axis=1,
        )

    down = jnp.zeros((y, features, zl * span), bf16)
    for k in range(y):
        moved = columns(k)
        if k:
            moved = lax.ppermute(moved, "y", step(y, k))
        down = lax.dynamic_update_slice_in_dim(down, moved[None], (y_here - k) % y, 0)
    down = down.reshape(y * features, zl * span)
    slot = slot_numbers(expert_ids, capacity)
    tail = jnp.pad(slot, ((0, 0), (0, 126)), constant_values=0).astype(bf16)
    seen = everyone(jnp.concatenate([tokens, tail], axis=1), ("zh", "zl"), zh * zl)
    seen = seen.reshape(zh, zl * block, width + 128)
    slot_seen = seen[0, :, width : width + 2].astype(f32).astype(jnp.int32)

    rows = zl * capacity
    wanted = (
        lax.axis_index("zh") * (x * capacity)
        + jnp.arange(x, dtype=jnp.int32)[:, None, None] * capacity
        + jnp.arange(capacity, dtype=jnp.int32)[None, None, :]
        + jnp.zeros((1, zl, 1), jnp.int32)
    ).reshape(-1)
    row_block = (jnp.arange(x * rows, dtype=jnp.int32) // capacity) % zl
    token_block = jnp.arange(zl * block, dtype=jnp.int32) // block
    hit = (slot_seen[:, 0][None, :] == wanted[:, None]) | (
        slot_seen[:, 1][None, :] == wanted[:, None]
    )
    hit = (hit & (row_block[:, None] == token_block[None, :])).astype(bf16)
    slots = jnp.concatenate(
        [
            jnp.dot(hit, seen[h, :, :width], preferred_element_type=f32)
            .astype(bf16)
            .reshape(x, rows, width)
            for h in range(zh)
        ],
        axis=1,
    )
    arrived = lax.all_to_all(slots, "x", 0, 0, tiled=True)
    arrived, down, gate_far, up_far = lax.optimization_barrier(
        (arrived, down, gate_far, up_far)
    )
    piece = jnp.concatenate(
        [arrived[i, h * rows : (h + 1) * rows] for h in range(zh) for i in range(x)],
        axis=1,
    )
    down_far = lax.ppermute(down, "c", SWAP)
    up1 = lax.ppermute(piece, "y", step(y, 1))
    dn1 = lax.ppermute(piece, "y", step(y, -1))
    half = rows // 2
    far_a = lax.ppermute(up1[:half], "y", step(y, 1))
    far_b = lax.ppermute(dn1[half:], "y", step(y, -1))
    blocks = (piece, up1, dn1, jnp.concatenate([far_a, far_b], axis=0))
    first = lax.axis_index("c") == 0

    def out(hidden, w):
        total = 0.0
        for k, h in enumerate(hidden):
            total = total + lax.dot_general(
                h,
                w[:, k * 2 * span : (k + 1) * 2 * span],
                (((1,), (1,)), ((), ())),
                preferred_element_type=f32,
            )
        return total.astype(bf16)

    core = lax.axis_index("c").astype(jnp.int32).reshape(1)
    hidden = gated(
        core, jnp.concatenate(blocks, axis=0), gate_own, up_own, gate_far, up_far
    )
    other = lax.ppermute(hidden, "zl", flip(zl, 4))
    pair = jnp.concatenate([hidden, other], axis=1)
    pairs = [pair] + [lax.ppermute(pair, "zl", flip(zl, k)) for k in (1, 2, 3)]
    both = jnp.concatenate(
        [jnp.where(first, down, down_far), jnp.where(first, down_far, down)], axis=0
    )
    part = out(pairs, both)
    parts = [part[n * rows : (n + 1) * rows] for n in range(y)]

    part = jnp.stack([parts[0], parts[2], parts[3], parts[1]])
    part = lax.dynamic_slice_in_dim(
        jnp.concatenate([part, part]), (y - y_here) % y, y, 0
    )
    part = lax.all_to_all(part, "y", 0, 0, tiled=True).astype(f32)
    result = ((part[0] + part[1]) + (part[2] + part[3])).astype(bf16)

    result = jnp.broadcast_to(
        result.reshape(1, zl, capacity * width), (zh, zl, capacity * width)
    ).reshape(zh * zl, capacity, width)
    result = lax.all_to_all(result, ("zh", "zl"), 0, 0, tiled=True)
    result = result.reshape(zh, zl, capacity, width)
    result = lax.dynamic_slice_in_dim(result, lax.axis_index("zh") * x, x, 1)
    result = jnp.concatenate([result[h] for h in range(zh)], axis=1)
    result = lax.all_to_all(result, "x", 0, 0, tiled=True)
    result, slot, gate_probs = lax.optimization_barrier((result, slot, gate_probs))
    result = result.reshape(experts * capacity, width)

    every = jnp.arange(experts * capacity, dtype=jnp.int32)
    every = (
        (every // capacity % zh) * (x * capacity)
        + (every // (zh * capacity)) * capacity
        + every % capacity
    )
    mixed = 0.0
    for k in range(2):
        pick = (slot[:, k][:, None] == every[None, :]).astype(bf16)
        picked = jnp.dot(pick, result, preferred_element_type=f32)
        mixed = mixed + gate_probs[:, k][:, None] * picked
    mixed = mixed.astype(bf16).reshape(block, c, y, features)
    return mixed.transpose(0, 2, 1, 3).reshape(block, width)


def solution(mesh):
    physical = Mesh(mesh.devices.reshape(SIZES), AXES)
    dp, expert = AXES[:3], AXES[3:]
    placed = (
        P(dp, expert),
        P(dp, None),
        P(dp, None),
        P(expert, None, dp),
        P(expert, None, dp),
        P(expert, dp, None),
    )
    return jax.shard_map(
        per_device,
        mesh=physical,
        in_specs=placed,
        out_specs=P(dp, expert),
        check_vma=False,
    )
```

```python
import jax
import jax.numpy as jnp
from jax import lax
from jax.experimental import pallas as pl
from jax.experimental.pallas import tpu as pltpu
from jax.sharding import Mesh, PartitionSpec as P

AXES = ("zl", "y", "c", "zh", "x")
SIZES = (8, 4, 2, 2, 4)
SWAP = [(0, 1), (1, 0)]


def step(count, shift):
    return [(i, (i + shift) % count) for i in range(count)]


def flip(axis_size, mask):
    return [(i, i ^ mask) for i in range(axis_size)]


def everyone(value, axis, count):
    return lax.all_to_all(
        jnp.broadcast_to(value[None], (count,) + value.shape), axis, 0, 0, tiled=True
    )


def slot_numbers(expert_ids, capacity):
    flat = expert_ids.reshape(-1)
    pairs = flat.shape[0]
    same = flat[:, None] == flat[None, :]
    index = jnp.arange(pairs, dtype=jnp.int32)
    earlier = index[None, :] < index[:, None]
    position = jnp.sum((same & earlier).astype(jnp.int32), axis=1)
    return (flat * capacity + position).reshape(expert_ids.shape)


DEPTH = 2048


def gated_kernel(core_ref, rows_ref, g0, u0, g1, u1, out_ref, gate, up):
    at = pl.program_id(0)

    @pl.when(at == 0)
    def _():
        gate[...] = jnp.zeros_like(gate)
        up[...] = jnp.zeros_like(up)

    lhs = rows_ref[...]
    w_g = jnp.concatenate([g0[...], g1[...]], axis=1)
    w_u = jnp.concatenate([u0[...], u1[...]], axis=1)
    gate[...] += jnp.dot(lhs, w_g, preferred_element_type=jnp.float32)
    up[...] += jnp.dot(lhs, w_u, preferred_element_type=jnp.float32)

    @pl.when(at == pl.num_programs(0) - 1)
    def _():
        g = gate[...]
        value = (g / (1.0 + jnp.exp(-g)) * up[...]).astype(out_ref.dtype)
        n = value.shape[1] // 2

        @pl.when(core_ref[0] == 0)
        def _():
            out_ref[...] = value

        @pl.when(core_ref[0] != 0)
        def _():
            out_ref[...] = jnp.concatenate([value[:, n:], value[:, :n]], axis=1)


def gated(core, rows, g0, u0, g1, u1):
    m, depth = rows.shape
    units = g0.shape[1]
    weight = pl.BlockSpec((DEPTH, units), lambda i, core: (i, 0))
    return pl.pallas_call(
        gated_kernel,
        out_shape=jax.ShapeDtypeStruct((m, 2 * units), rows.dtype),
        grid_spec=pltpu.PrefetchScalarGridSpec(
            num_scalar_prefetch=1,
            grid=(depth // DEPTH,),
            in_specs=[pl.BlockSpec((m, DEPTH), lambda i, core: (0, i))] + [weight] * 4,
            out_specs=pl.BlockSpec((m, 2 * units), lambda i, core: (0, 0)),
            scratch_shapes=[
                pltpu.VMEM((m, 2 * units), jnp.float32),
                pltpu.VMEM((m, 2 * units), jnp.float32),
            ],
        ),
        compiler_params=pltpu.CompilerParams(dimension_semantics=("arbitrary",)),
        cost_estimate=pl.CostEstimate(
            flops=2 * m * depth * units * 4,
            transcendentals=m * units * 2,
            bytes_accessed=depth * (m + 4 * units) * 2,
        ),
        name="gated",
    )(core, rows, g0, u0, g1, u1)


def per_device(tokens, expert_ids, gate_probs, w_gate, w_up, w_down_t):
    zl, y, c, zh, x = SIZES
    block, width = tokens.shape
    capacity = block // 2
    experts = zh * x
    model = width * experts
    units = w_gate.shape[2]
    f32, bf16 = jnp.float32, jnp.bfloat16

    gate_own, up_own = w_gate[0], w_up[0]
    gate_far = lax.ppermute(gate_own, "c", SWAP)
    up_far = lax.ppermute(up_own, "c", SWAP)
    features = w_down_t.shape[1]
    z_here = lax.axis_index("zl")
    order = range(zl)
    span = c * units
    y_here = lax.axis_index("y")

    def columns(shift):
        at = ((y_here + shift) % y) * span
        return jnp.concatenate(
            [
                lax.dynamic_slice_in_dim(
                    w_down_t[0], (z_here ^ j) * (y * span) + at, span, 1
                )
                for j in order
            ],
            axis=1,
        )

    down = jnp.zeros((y, features, zl * span), bf16)
    for k in range(y):
        moved = columns(k)
        if k:
            moved = lax.ppermute(moved, "y", step(y, k))
        down = lax.dynamic_update_slice_in_dim(down, moved[None], (y_here - k) % y, 0)
    down = down.reshape(y * features, zl * span)
    slot = slot_numbers(expert_ids, capacity)
    tail = jnp.pad(slot, ((0, 0), (0, 126)), constant_values=0).astype(bf16)
    seen = everyone(jnp.concatenate([tokens, tail], axis=1), ("zh", "zl"), zh * zl)
    seen = seen.reshape(zh, zl * block, width + 128)
    slot_seen = seen[0, :, width : width + 2].astype(f32).astype(jnp.int32)

    rows = zl * capacity
    wanted = (
        lax.axis_index("zh") * (x * capacity)
        + jnp.arange(x, dtype=jnp.int32)[:, None, None] * capacity
        + jnp.arange(capacity, dtype=jnp.int32)[None, None, :]
        + jnp.zeros((1, zl, 1), jnp.int32)
    ).reshape(-1)
    row_block = (jnp.arange(x * rows, dtype=jnp.int32) // capacity) % zl
    token_block = jnp.arange(zl * block, dtype=jnp.int32) // block
    hit = (slot_seen[:, 0][None, :] == wanted[:, None]) | (
        slot_seen[:, 1][None, :] == wanted[:, None]
    )
    hit = (hit & (row_block[:, None] == token_block[None, :])).astype(bf16)
    slots = jnp.concatenate(
        [
            jnp.dot(hit, seen[h, :, :width], preferred_element_type=f32)
            .astype(bf16)
            .reshape(x, rows, width)
            for h in range(zh)
        ],
        axis=1,
    )
    arrived = lax.all_to_all(slots, "x", 0, 0, tiled=True)
    arrived, down, gate_far, up_far = lax.optimization_barrier(
        (arrived, down, gate_far, up_far)
    )
    piece = jnp.concatenate(
        [arrived[i, h * rows : (h + 1) * rows] for h in range(zh) for i in range(x)],
        axis=1,
    )
    down_far = lax.ppermute(down, "c", SWAP)
    up1 = lax.ppermute(piece, "y", step(y, 1))
    dn1 = lax.ppermute(piece, "y", step(y, -1))
    half = rows // 2
    far_a = lax.ppermute(up1[:half], "y", step(y, 1))
    far_b = lax.ppermute(dn1[half:], "y", step(y, -1))
    blocks = (piece, up1, dn1, far_a, far_b)
    first = lax.axis_index("c") == 0

    def out(hidden, w):
        total = 0.0
        for k, h in enumerate(hidden):
            total = total + lax.dot_general(
                h,
                w[:, k * span : (k + 1) * span],
                (((1,), (1,)), ((), ())),
                preferred_element_type=f32,
            )
        return total.astype(bf16)

    core = lax.axis_index("c").astype(jnp.int32).reshape(1)
    hidden = gated(
        core, jnp.concatenate(blocks, axis=0), gate_own, up_own, gate_far, up_far
    )
    other = lax.ppermute(hidden, "zl", flip(zl, 4))
    near = [lax.ppermute(hidden, "zl", flip(zl, k)) for k in (1, 2, 3)]
    distant = [lax.ppermute(other, "zl", flip(zl, k)) for k in (1, 2, 3)]
    pairs = [hidden, *near, other, *distant]
    both = jnp.concatenate(
        [jnp.where(first, down, down_far), jnp.where(first, down_far, down)], axis=0
    )
    part = out(pairs, both)
    parts = [part[n * rows : (n + 1) * rows] for n in range(y)]

    part = jnp.stack([parts[0], parts[2], parts[3], parts[1]])
    part = lax.dynamic_slice_in_dim(
        jnp.concatenate([part, part]), (y - y_here) % y, y, 0
    )
    part = lax.all_to_all(part, "y", 0, 0, tiled=True).astype(f32)
    result = ((part[0] + part[1]) + (part[2] + part[3])).astype(bf16)

    result = jnp.broadcast_to(
        result.reshape(1, zl, capacity * width), (zh, zl, capacity * width)
    ).reshape(zh * zl, capacity, width)
    result = lax.all_to_all(result, ("zh", "zl"), 0, 0, tiled=True)
    result = result.reshape(zh, zl, capacity, width)
    result = lax.dynamic_slice_in_dim(result, lax.axis_index("zh") * x, x, 1)
    result = jnp.concatenate([result[h] for h in range(zh)], axis=1)
    result = lax.all_to_all(result, "x", 0, 0, tiled=True)
    result, slot, gate_probs = lax.optimization_barrier((result, slot, gate_probs))
    result = result.reshape(experts * capacity, width)

    every = jnp.arange(experts * capacity, dtype=jnp.int32)
    every = (
        (every // capacity % zh) * (x * capacity)
        + (every // (zh * capacity)) * capacity
        + every % capacity
    )
    mixed = 0.0
    for k in range(2):
        pick = (slot[:, k][:, None] == every[None, :]).astype(bf16)
        picked = jnp.dot(pick, result, preferred_element_type=f32)
        mixed = mixed + gate_probs[:, k][:, None] * picked
    mixed = mixed.astype(bf16).reshape(block, c, y, features)
    return mixed.transpose(0, 2, 1, 3).reshape(block, width)


def solution(mesh):
    physical = Mesh(mesh.devices.reshape(SIZES), AXES)
    dp, expert = AXES[:3], AXES[3:]
    placed = (
        P(dp, expert),
        P(dp, None),
        P(dp, None),
        P(expert, None, dp),
        P(expert, None, dp),
        P(expert, dp, None),
    )
    return jax.shard_map(
        per_device,
        mesh=physical,
        in_specs=placed,
        out_specs=P(dp, expert),
        check_vma=False,
    )
```

```python
import functools

import jax
import jax.numpy as jnp
from jax import lax
from jax.experimental import pallas as pl
from jax.experimental.pallas import tpu as pltpu
from jax.sharding import Mesh, PartitionSpec as P

AXES = ("zl", "y", "c", "zh", "x")
SIZES = (8, 4, 2, 2, 4)
SWAP = [(0, 1), (1, 0)]


def step(count, shift):
    return [(i, (i + shift) % count) for i in range(count)]


def flip(axis_size, mask):
    return [(i, i ^ mask) for i in range(axis_size)]


def numbered_kernel(ids_ref, tokens_ref, copies_ref, slot_ref, *, capacity):
    block, width = tokens_ref.shape
    row = lax.broadcasted_iota(jnp.int32, (block, block), 0)
    column = lax.broadcasted_iota(jnp.int32, (block, block), 1)
    named = [jnp.broadcast_to(ids_ref[k : k + 1, :], (block, block)) for k in range(2)]
    lane = lax.broadcasted_iota(jnp.int32, (block, 128), 1)
    tail = jnp.zeros((block, 128), jnp.int32)
    for k in range(2):
        mine = jnp.sum(jnp.where(row == column, named[k], 0), axis=1, keepdims=True)
        same = (named[0] == mine).astype(jnp.int32) + (named[1] == mine).astype(jnp.int32)
        earlier = jnp.sum(jnp.where(column < row, same, 0), axis=1, keepdims=True)
        tail = jnp.where(lane == k, mine * capacity + earlier, tail)
    slot_ref[...] = tail
    whole = jnp.concatenate(
        [tokens_ref[...], tail.astype(jnp.float32).astype(tokens_ref.dtype)], axis=1
    )
    copies_ref[...] = jnp.broadcast_to(whole[None], copies_ref.shape)


def numbered(expert_ids, tokens, capacity, copies):
    block, width = tokens.shape
    return pl.pallas_call(
        functools.partial(numbered_kernel, capacity=capacity),
        out_shape=(
            jax.ShapeDtypeStruct((copies, block, width + 128), tokens.dtype),
            jax.ShapeDtypeStruct((block, 128), jnp.int32),
        ),
        name="numbered",
    )(expert_ids.T, tokens)


def dealt_kernel(at_ref, w_ref, *out_refs, span):
    count = len(out_refs)
    for k, out_ref in enumerate(out_refs):
        to = lax.rem(at_ref[0] + k, count)
        for j in range(out_ref.shape[1] // span):
            z = at_ref[1] ^ j
            at = pl.multiple_of((z * count + to) * span, span)
            out_ref[:, j * span : (j + 1) * span] = w_ref[0, :, pl.ds(at, span)]


def dealt(y_here, z_here, w, count, span):
    _, rows, units = w.shape
    return pl.pallas_call(
        functools.partial(dealt_kernel, span=span),
        out_shape=[jax.ShapeDtypeStruct((rows, units // count), w.dtype)] * count,
        in_specs=[
            pl.BlockSpec(memory_space=pltpu.SMEM),
            pl.BlockSpec(memory_space=pltpu.VMEM),
        ],
        out_specs=[pl.BlockSpec(memory_space=pltpu.VMEM)] * count,
        cost_estimate=pl.CostEstimate(
            flops=4_000_000, transcendentals=0, bytes_accessed=rows * units * 4
        ),
        name="dealt",
    )(jnp.stack([y_here, z_here]).astype(jnp.int32), w)


DEPTH = 2048


def gated_kernel(core_ref, rows_ref, g0, u0, g1, u1, out_ref, gate, up):
    at = pl.program_id(0)

    @pl.when(at == 0)
    def _():
        gate[...] = jnp.zeros_like(gate)
        up[...] = jnp.zeros_like(up)

    lhs = rows_ref[...]
    w_g = jnp.concatenate([g0[...], g1[...]], axis=1)
    w_u = jnp.concatenate([u0[...], u1[...]], axis=1)
    gate[...] += jnp.dot(lhs, w_g, preferred_element_type=jnp.float32)
    up[...] += jnp.dot(lhs, w_u, preferred_element_type=jnp.float32)

    @pl.when(at == pl.num_programs(0) - 1)
    def _():
        g = gate[...]
        value = (g / (1.0 + jnp.exp(-g)) * up[...]).astype(out_ref.dtype)
        n = value.shape[1] // 2

        @pl.when(core_ref[0] == 0)
        def _():
            out_ref[...] = value

        @pl.when(core_ref[0] != 0)
        def _():
            out_ref[...] = jnp.concatenate([value[:, n:], value[:, :n]], axis=1)


def gated(core, rows, g0, u0, g1, u1):
    m, depth = rows.shape
    units = g0.shape[1]
    weight = pl.BlockSpec((DEPTH, units), lambda i, core: (i, 0))
    return pl.pallas_call(
        gated_kernel,
        out_shape=jax.ShapeDtypeStruct((m, 2 * units), rows.dtype),
        grid_spec=pltpu.PrefetchScalarGridSpec(
            num_scalar_prefetch=1,
            grid=(depth // DEPTH,),
            in_specs=[pl.BlockSpec((m, DEPTH), lambda i, core: (0, i))] + [weight] * 4,
            out_specs=pl.BlockSpec((m, 2 * units), lambda i, core: (0, 0)),
            scratch_shapes=[
                pltpu.VMEM((m, 2 * units), jnp.float32),
                pltpu.VMEM((m, 2 * units), jnp.float32),
            ],
        ),
        compiler_params=pltpu.CompilerParams(dimension_semantics=("arbitrary",)),
        cost_estimate=pl.CostEstimate(
            flops=2 * m * depth * units * 4,
            transcendentals=m * units * 2,
            bytes_accessed=depth * (m + 4 * units) * 2,
        ),
        name="gated",
    )(core, rows, g0, u0, g1, u1)


def per_device(tokens, expert_ids, gate_probs, w_gate, w_up, w_down_t):
    zl, y, c, zh, x = SIZES
    block, width = tokens.shape
    capacity = block // 2
    experts = zh * x
    model = width * experts
    units = w_gate.shape[2]
    f32, bf16 = jnp.float32, jnp.bfloat16

    gate_own, up_own = w_gate[0], w_up[0]
    gate_far = lax.ppermute(gate_own, "c", SWAP)
    up_far = lax.ppermute(up_own, "c", SWAP)
    features = w_down_t.shape[1]
    z_here = lax.axis_index("zl")
    span = c * units
    y_here = lax.axis_index("y")

    columns = dealt(y_here, z_here, w_down_t, y, span)
    down = jnp.zeros((y, features, zl * span), bf16)
    for k in range(y):
        moved = columns[k]
        if k:
            moved = lax.ppermute(moved, "y", step(y, k))
        down = lax.dynamic_update_slice_in_dim(down, moved[None], (y_here - k) % y, 0)
    down = down.reshape(y * features, zl * span)
    copies, slot = numbered(expert_ids, tokens, capacity, zh * zl)
    seen = lax.all_to_all(copies, ("zh", "zl"), 0, 0, tiled=True)
    seen = seen.reshape(zh, zl * block, width + 128)
    slot_seen = seen[0, :, width : width + 2].astype(f32).astype(jnp.int32)

    rows = zl * capacity
    wanted = (
        lax.axis_index("zh") * (x * capacity)
        + jnp.arange(x, dtype=jnp.int32)[:, None, None] * capacity
        + jnp.arange(capacity, dtype=jnp.int32)[None, None, :]
        + jnp.zeros((1, zl, 1), jnp.int32)
    ).reshape(-1)
    row_block = (jnp.arange(x * rows, dtype=jnp.int32) // capacity) % zl
    token_block = jnp.arange(zl * block, dtype=jnp.int32) // block
    hit = (slot_seen[:, 0][None, :] == wanted[:, None]) | (
        slot_seen[:, 1][None, :] == wanted[:, None]
    )
    hit = (hit & (row_block[:, None] == token_block[None, :])).astype(bf16)
    slots = jnp.concatenate(
        [
            jnp.dot(hit, seen[h, :, :width], preferred_element_type=f32)
            .astype(bf16)
            .reshape(x, rows, width)
            for h in range(zh)
        ],
        axis=1,
    )
    arrived = lax.all_to_all(slots, "x", 0, 0, tiled=True)
    arrived, down, gate_far, up_far = lax.optimization_barrier(
        (arrived, down, gate_far, up_far)
    )
    piece = jnp.concatenate(
        [arrived[i, h * rows : (h + 1) * rows] for h in range(zh) for i in range(x)],
        axis=1,
    )
    down_far = lax.ppermute(down, "c", SWAP)
    up1 = lax.ppermute(piece, "y", step(y, 1))
    dn1 = lax.ppermute(piece, "y", step(y, -1))
    half = rows // 2
    far_a = lax.ppermute(up1[:half], "y", step(y, 1))
    far_b = lax.ppermute(dn1[half:], "y", step(y, -1))
    blocks = (piece, up1, dn1, far_a, far_b)
    first = lax.axis_index("c") == 0

    def out(hidden, w):
        total = 0.0
        for k, h in enumerate(hidden):
            total = total + lax.dot_general(
                h,
                w[:, k * span : (k + 1) * span],
                (((1,), (1,)), ((), ())),
                preferred_element_type=f32,
            )
        return total.astype(bf16)

    core = lax.axis_index("c").astype(jnp.int32).reshape(1)
    hidden = gated(
        core, jnp.concatenate(blocks, axis=0), gate_own, up_own, gate_far, up_far
    )
    other = lax.ppermute(hidden, "zl", flip(zl, 4))
    near = [lax.ppermute(hidden, "zl", flip(zl, k)) for k in (1, 2, 3)]
    distant = [lax.ppermute(other, "zl", flip(zl, k)) for k in (1, 2, 3)]
    pairs = [hidden, *near, other, *distant]
    own = down.reshape(y, features, zl * span)
    far = down_far.reshape(y, features, zl * span)
    both = jnp.stack(
        [jnp.where(first, own, far), jnp.where(first, far, own)], axis=1
    ).reshape(width, zl * span)
    part = out(pairs, both)
    parts = [part[n * rows : (n + 1) * rows] for n in range(y)]

    part = jnp.stack([parts[0], parts[2], parts[3], parts[1]])
    part = lax.dynamic_slice_in_dim(
        jnp.concatenate([part, part]), (y - y_here) % y, y, 0
    )
    part = lax.all_to_all(part, "y", 0, 0, tiled=True).astype(f32)
    result = ((part[0] + part[1]) + (part[2] + part[3])).astype(bf16)

    result = jnp.broadcast_to(
        result.reshape(1, zl, capacity * width), (zh, zl, capacity * width)
    ).reshape(zh * zl, capacity, width)
    result = lax.all_to_all(result, ("zh", "zl"), 0, 0, tiled=True)
    result = result.reshape(zh, zl, capacity, width)
    result = lax.dynamic_slice_in_dim(result, lax.axis_index("zh") * x, x, 1)
    result = jnp.concatenate([result[h] for h in range(zh)], axis=1)
    result = lax.all_to_all(result, "x", 0, 0, tiled=True)
    result, slot, gate_probs = lax.optimization_barrier((result, slot, gate_probs))
    result = result.reshape(experts * capacity, width)

    every = jnp.arange(experts * capacity, dtype=jnp.int32)
    every = (
        (every // capacity % zh) * (x * capacity)
        + (every // (zh * capacity)) * capacity
        + every % capacity
    )
    mixed = 0.0
    for k in range(2):
        pick = (slot[:, k][:, None] == every[None, :]).astype(bf16)
        picked = jnp.dot(pick, result, preferred_element_type=f32)
        mixed = mixed + gate_probs[:, k][:, None] * picked
    return mixed.astype(bf16)


def solution(mesh):
    physical = Mesh(mesh.devices.reshape(SIZES), AXES)
    dp, expert = AXES[:3], AXES[3:]
    placed = (
        P(dp, expert),
        P(dp, None),
        P(dp, None),
        P(expert, None, dp),
        P(expert, None, dp),
        P(expert, dp, None),
    )
    return jax.shard_map(
        per_device,
        mesh=physical,
        in_specs=placed,
        out_specs=P(dp, expert),
        check_vma=False,
    )
```

```python
import functools

import jax
import jax.numpy as jnp
from jax import lax
from jax.experimental import pallas as pl
from jax.experimental.pallas import tpu as pltpu
from jax.sharding import Mesh, PartitionSpec as P

AXES = ("zl", "y", "c", "zh", "x")
SIZES = (8, 4, 2, 2, 4)
SWAP = [(0, 1), (1, 0)]


def step(count, shift):
    return [(i, (i + shift) % count) for i in range(count)]


def flip(axis_size, mask):
    return [(i, i ^ mask) for i in range(axis_size)]


def numbered_kernel(ids_ref, tokens_ref, copies_ref, slot_ref, *, capacity):
    block, width = tokens_ref.shape
    row = lax.broadcasted_iota(jnp.int32, (block, block), 0)
    column = lax.broadcasted_iota(jnp.int32, (block, block), 1)
    named = [jnp.broadcast_to(ids_ref[k : k + 1, :], (block, block)) for k in range(2)]
    lane = lax.broadcasted_iota(jnp.int32, (block, 128), 1)
    tail = jnp.zeros((block, 128), jnp.int32)
    for k in range(2):
        mine = jnp.sum(jnp.where(row == column, named[k], 0), axis=1, keepdims=True)
        same = (named[0] == mine).astype(jnp.int32) + (named[1] == mine).astype(jnp.int32)
        earlier = jnp.sum(jnp.where(column < row, same, 0), axis=1, keepdims=True)
        tail = jnp.where(lane == k, mine * capacity + earlier, tail)
    slot_ref[...] = tail
    whole = jnp.concatenate(
        [tokens_ref[...], tail.astype(jnp.float32).astype(tokens_ref.dtype)], axis=1
    )
    copies_ref[...] = jnp.broadcast_to(whole[None], copies_ref.shape)


def numbered(expert_ids, tokens, capacity, copies):
    block, width = tokens.shape
    return pl.pallas_call(
        functools.partial(numbered_kernel, capacity=capacity),
        out_shape=(
            jax.ShapeDtypeStruct((copies, block, width + 128), tokens.dtype),
            jax.ShapeDtypeStruct((block, 128), jnp.int32),
        ),
        name="numbered",
    )(expert_ids.T, tokens)


def dealt_kernel(at_ref, w_ref, *out_refs, span):
    count = len(out_refs)
    for k, out_ref in enumerate(out_refs):
        to = lax.rem(at_ref[0] + k, count)
        for j in range(out_ref.shape[1] // span):
            z = at_ref[1] ^ j
            at = pl.multiple_of((z * count + to) * span, span)
            out_ref[:, j * span : (j + 1) * span] = w_ref[0, :, pl.ds(at, span)]


def dealt(y_here, z_here, w, count, span):
    _, rows, units = w.shape
    return pl.pallas_call(
        functools.partial(dealt_kernel, span=span),
        out_shape=[jax.ShapeDtypeStruct((rows, units // count), w.dtype)] * count,
        in_specs=[
            pl.BlockSpec(memory_space=pltpu.SMEM),
            pl.BlockSpec(memory_space=pltpu.VMEM),
        ],
        out_specs=[pl.BlockSpec(memory_space=pltpu.VMEM)] * count,
        cost_estimate=pl.CostEstimate(
            flops=4_000_000, transcendentals=0, bytes_accessed=rows * units * 4
        ),
        name="dealt",
    )(jnp.stack([y_here, z_here]).astype(jnp.int32), w)


DEPTH = 3072


def gated_kernel(core_ref, rows_ref, g0, u0, g1, u1, out_ref, gate, up):
    at = pl.program_id(0)

    @pl.when(at == 0)
    def _():
        gate[...] = jnp.zeros_like(gate)
        up[...] = jnp.zeros_like(up)

    lhs = rows_ref[...]
    w_g = jnp.concatenate([g0[...], g1[...]], axis=1)
    w_u = jnp.concatenate([u0[...], u1[...]], axis=1)
    gate[...] += jnp.dot(lhs, w_g, preferred_element_type=jnp.float32)
    up[...] += jnp.dot(lhs, w_u, preferred_element_type=jnp.float32)

    @pl.when(at == pl.num_programs(0) - 1)
    def _():
        g = gate[...]
        value = (g / (1.0 + jnp.exp(-g)) * up[...]).astype(out_ref.dtype)
        n = value.shape[1] // 2

        @pl.when(core_ref[0] == 0)
        def _():
            out_ref[...] = value

        @pl.when(core_ref[0] != 0)
        def _():
            out_ref[...] = jnp.concatenate([value[:, n:], value[:, :n]], axis=1)


def gated(core, rows, g0, u0, g1, u1):
    m, depth = rows.shape
    units = g0.shape[1]
    weight = pl.BlockSpec((DEPTH, units), lambda i, core: (i, 0))
    return pl.pallas_call(
        gated_kernel,
        out_shape=jax.ShapeDtypeStruct((m, 2 * units), rows.dtype),
        grid_spec=pltpu.PrefetchScalarGridSpec(
            num_scalar_prefetch=1,
            grid=(depth // DEPTH,),
            in_specs=[pl.BlockSpec((m, DEPTH), lambda i, core: (0, i))] + [weight] * 4,
            out_specs=pl.BlockSpec((m, 2 * units), lambda i, core: (0, 0)),
            scratch_shapes=[
                pltpu.VMEM((m, 2 * units), jnp.float32),
                pltpu.VMEM((m, 2 * units), jnp.float32),
            ],
        ),
        compiler_params=pltpu.CompilerParams(dimension_semantics=("arbitrary",)),
        cost_estimate=pl.CostEstimate(
            flops=2 * m * depth * units * 4,
            transcendentals=m * units * 2,
            bytes_accessed=depth * (m + 4 * units) * 2,
        ),
        name="gated",
    )(core, rows, g0, u0, g1, u1)


def per_device(tokens, expert_ids, gate_probs, w_gate, w_up, w_down_t):
    zl, y, c, zh, x = SIZES
    block, width = tokens.shape
    capacity = block // 2
    experts = zh * x
    model = width * experts
    units = w_gate.shape[2]
    f32, bf16 = jnp.float32, jnp.bfloat16

    gate_own, up_own = w_gate[0], w_up[0]
    gate_far = lax.ppermute(gate_own, "c", SWAP)
    up_far = lax.ppermute(up_own, "c", SWAP)
    features = w_down_t.shape[1]
    z_here = lax.axis_index("zl")
    span = c * units
    y_here = lax.axis_index("y")

    columns = dealt(y_here, z_here, w_down_t, y, span)
    down = jnp.zeros((y, features, zl * span), bf16)
    for k in range(y):
        moved = columns[k]
        if k:
            moved = lax.ppermute(moved, "y", step(y, k))
        down = lax.dynamic_update_slice_in_dim(down, moved[None], (y_here - k) % y, 0)
    down = down.reshape(y * features, zl * span)
    copies, slot = numbered(expert_ids, tokens, capacity, zh * zl)
    seen = lax.all_to_all(copies, ("zh", "zl"), 0, 0, tiled=True)
    seen = seen.reshape(zh, zl * block, width + 128)
    slot_seen = seen[0, :, width : width + 2].astype(f32).astype(jnp.int32)

    rows = zl * capacity
    wanted = (
        lax.axis_index("zh") * (x * capacity)
        + jnp.arange(x, dtype=jnp.int32)[:, None, None] * capacity
        + jnp.arange(capacity, dtype=jnp.int32)[None, None, :]
        + jnp.zeros((1, zl, 1), jnp.int32)
    ).reshape(-1)
    row_block = (jnp.arange(x * rows, dtype=jnp.int32) // capacity) % zl
    token_block = jnp.arange(zl * block, dtype=jnp.int32) // block
    hit = (slot_seen[:, 0][None, :] == wanted[:, None]) | (
        slot_seen[:, 1][None, :] == wanted[:, None]
    )
    hit = (hit & (row_block[:, None] == token_block[None, :])).astype(bf16)
    slots = jnp.concatenate(
        [
            jnp.dot(hit, seen[h, :, :width], preferred_element_type=f32)
            .astype(bf16)
            .reshape(x, rows, width)
            for h in range(zh)
        ],
        axis=1,
    )
    arrived = lax.all_to_all(slots, "x", 0, 0, tiled=True)
    arrived, down, gate_far, up_far = lax.optimization_barrier(
        (arrived, down, gate_far, up_far)
    )
    piece = jnp.concatenate(
        [arrived[i, h * rows : (h + 1) * rows] for h in range(zh) for i in range(x)],
        axis=1,
    )
    down_far = lax.ppermute(down, "c", SWAP)
    up1 = lax.ppermute(piece, "y", step(y, 1))
    dn1 = lax.ppermute(piece, "y", step(y, -1))
    half = rows // 2
    far_a = lax.ppermute(up1[:half], "y", step(y, 1))
    far_b = lax.ppermute(dn1[half:], "y", step(y, -1))
    blocks = (piece, up1, dn1, far_a, far_b)
    first = lax.axis_index("c") == 0

    def out(hidden, w):
        total = 0.0
        for k, h in enumerate(hidden):
            total = total + lax.dot_general(
                h,
                w[:, k * span : (k + 1) * span],
                (((1,), (1,)), ((), ())),
                preferred_element_type=f32,
            )
        return total.astype(bf16)

    core = lax.axis_index("c").astype(jnp.int32).reshape(1)
    hidden = gated(
        core, jnp.concatenate(blocks, axis=0), gate_own, up_own, gate_far, up_far
    )
    other = lax.ppermute(hidden, "zl", flip(zl, 4))
    near = [lax.ppermute(hidden, "zl", flip(zl, k)) for k in (1, 2, 3)]
    distant = [lax.ppermute(other, "zl", flip(zl, k)) for k in (1, 2, 3)]
    pairs = [hidden, *near, other, *distant]
    own = down.reshape(y, features, zl * span)
    far = down_far.reshape(y, features, zl * span)
    both = jnp.stack(
        [jnp.where(first, own, far), jnp.where(first, far, own)], axis=1
    ).reshape(width, zl * span)
    part = out(pairs, both)
    parts = [part[n * rows : (n + 1) * rows] for n in range(y)]

    part = jnp.stack([parts[0], parts[2], parts[3], parts[1]])
    part = lax.dynamic_slice_in_dim(
        jnp.concatenate([part, part]), (y - y_here) % y, y, 0
    )
    part = lax.all_to_all(part, "y", 0, 0, tiled=True).astype(f32)
    result = ((part[0] + part[1]) + (part[2] + part[3])).astype(bf16)

    result = jnp.broadcast_to(
        result.reshape(1, zl, capacity * width), (zh, zl, capacity * width)
    ).reshape(zh * zl, capacity, width)
    result = lax.all_to_all(result, ("zh", "zl"), 0, 0, tiled=True)
    result = result.reshape(zh, zl, capacity, width)
    result = lax.dynamic_slice_in_dim(result, lax.axis_index("zh") * x, x, 1)
    result = jnp.concatenate([result[h] for h in range(zh)], axis=1)
    result = lax.all_to_all(result, "x", 0, 0, tiled=True)
    result, slot, gate_probs = lax.optimization_barrier((result, slot, gate_probs))
    result = result.reshape(experts * capacity, width)

    every = jnp.arange(experts * capacity, dtype=jnp.int32)
    every = (
        (every // capacity % zh) * (x * capacity)
        + (every // (zh * capacity)) * capacity
        + every % capacity
    )
    mixed = 0.0
    for k in range(2):
        pick = (slot[:, k][:, None] == every[None, :]).astype(bf16)
        picked = jnp.dot(pick, result, preferred_element_type=f32)
        mixed = mixed + gate_probs[:, k][:, None] * picked
    return mixed.astype(bf16)


def solution(mesh):
    physical = Mesh(mesh.devices.reshape(SIZES), AXES)
    dp, expert = AXES[:3], AXES[3:]
    placed = (
        P(dp, expert),
        P(dp, None),
        P(dp, None),
        P(expert, None, dp),
        P(expert, None, dp),
        P(expert, dp, None),
    )
    return jax.shard_map(
        per_device,
        mesh=physical,
        in_specs=placed,
        out_specs=P(dp, expert),
        check_vma=False,
    )
```
